32 devices in a mesh: face: 16 (over z, y, core), sub: 2 (over x).
Axes of the slice: x: 2, y: 2, z: 4, core: 2. Of those that a mesh axis runs over, the one named last changes fastest.
Arguments:
- prognostic: bfloat16 [3, 2048, 16, 128], P(None, ('face', 'sub')), may hold values from -4 to 4
- metric: float32 [4, 2048, 16], P(None, ('face', 'sub')), may hold values from -0.35 to 1.6, as said below
- coriolis: float32 [2048, 16], P(('face', 'sub')), may hold values from -1.5 to 1.5
- node_point: int32 [2048, 16], P(('face', 'sub')), may hold values from 0 to 678, as said below
- send_point: int32 [6784], P(('face', 'sub')), may hold values from 0 to 678, as said below
- recv_point: int32 [6784], P(('face', 'sub')), may hold values from 0 to 678, as said below
Outputs:
- advanced: bfloat16 [3, 2048, 16, 128], P(None, ('face', 'sub'))
The draws below stay inside these ranges and needn't reach their ends.
Inputs may be any that keep to these rules, and one draw needn't show every extreme that they name: `node_point`: each device's numbers are its 679 local points; element nodes that are the same point of the surface on one device carry the same number. `send_point`: on every device the 212 slots form groups in this order: 7 slots of offset +1, 7 of offset -1, 97 of offset +8, 97 of offset -8, then one slot each of offsets 8 + 1, -8 - 1, 7, 1 - 8. A slot names the sender's point that the device at curve index d + o, taken modulo 32, shares. Every slot is used. `recv_point`: slot s of device d names the local point that is the same surface point as the sender's slot s, the sender being the device at d minus the slot's group offset modulo 32. The copies of every shared point are linked between every two devices that hold them. `metric`: entries 0 and 3 lie in [0.6, 1.6], entries 1 and 2 in [-0.35, 0.35].
All inputs are finite; a program needn't handle non-finite values.
Results may differ from the reference program's by a relative error of at most 0.007.
Values sent between devices are 32-bit elements; how exact they have to be, the bound alone decides.
A program may use at most 64 MiB of HBM per device.

```python
import math
import jax
import jax.numpy as jnp
import numpy as np
from jax import lax

BX = 32
BY = 2
LEV = 128
ELEMS = 64
BLOCKS = 32
ELEMENTS = 2048
LAP = 8
PTS = 679
LINKS = 212


def link_grid_points():
    grid_width = 3 * BX + 1
    grid_height = 3 * BY + 1
    sender = []
    receiver = []
    for height in range(grid_height):
        sender.append(height * grid_width + 3 * BX)
        receiver.append(height * grid_width)
    for height in range(grid_height):
        sender.append(height * grid_width)
        receiver.append(height * grid_width + 3 * BX)
    for column in range(grid_width):
        sender.append(3 * BY * grid_width + column)
        receiver.append(column)
    for column in range(grid_width):
        sender.append(column)
        receiver.append(3 * BY * grid_width + column)
    sender.append(3 * BY * grid_width + 3 * BX)
    receiver.append(0)
    sender.append(0)
    receiver.append(3 * BY * grid_width + 3 * BX)
    sender.append(3 * BY * grid_width)
    receiver.append(3 * BX)
    sender.append(3 * BX)
    receiver.append(3 * BY * grid_width)
    return (np.array(sender, np.int32), np.array(receiver, np.int32))


def mesh_tables(key):
    base = jax.random.fold_in(key, 4242)
    key_elem, key_rot, key_point = jax.random.split(base, 3)
    elements = BX * BY
    placement_order = jax.vmap(lambda sub_key: jax.random.permutation(sub_key, elements))(jax.random.split(key_elem, BLOCKS)).astype(jnp.int32)
    rotation = jax.random.randint(key_rot, (BLOCKS, elements), 0, 4).astype(jnp.int32)[..., None]
    relabel = jax.vmap(lambda sub_key: jax.random.permutation(sub_key, PTS))(jax.random.split(key_point, BLOCKS)).astype(jnp.int32)
    across = placement_order % BX
    upward = placement_order // BX
    node_index = jnp.arange(16, dtype=jnp.int32)
    node_row = node_index // 4
    node_col = node_index % 4
    rot_col = jnp.where(rotation == 0, node_col, jnp.where(rotation == 1, 3 - node_row, jnp.where(rotation == 2, 3 - node_col, node_row)))
    rot_row = jnp.where(rotation == 0, node_row, jnp.where(rotation == 1, node_col, jnp.where(rotation == 2, 3 - node_row, 3 - node_col)))
    grid_index = (3 * upward[..., None] + rot_row) * (3 * BX + 1) + 3 * across[..., None] + rot_col
    node_table = jnp.take_along_axis(relabel, grid_index.reshape(BLOCKS, elements * 16).astype(jnp.int32), axis=1)
    sender, receiver = link_grid_points()
    send_table = relabel[:, jnp.asarray(sender)].reshape(-1).astype(jnp.int32)
    recv_table = relabel[:, jnp.asarray(receiver)].reshape(-1).astype(jnp.int32)
    return (node_table.reshape(ELEMENTS, 16).astype(jnp.int32), send_table, recv_table)


def draw_node_point(key, part):
    return mesh_tables(key)[0]


def draw_send_point(key, part):
    return mesh_tables(key)[1]


def draw_recv_point(key, part):
    return mesh_tables(key)[2]


def draw_metric(key, part):
    key_diag, key_off = jax.random.split(jax.random.fold_in(key, 17), 2)
    diagonal = jnp.exp(jax.random.uniform(key_diag, (2, ELEMENTS, 16), jnp.float32, math.log(0.6), math.log(1.6)))
    off_diag = jax.random.uniform(key_off, (2, ELEMENTS, 16), jnp.float32, -0.35, 0.35)
    diagonal = jnp.clip(diagonal, 0.6, 1.6)
    return jnp.stack([diagonal[0], off_diag[0], off_diag[1], diagonal[1]]).astype(jnp.float32)


def block_levels(own_key, shape, cuts, least, high):
    level, own = 1.0, jax.random.fold_in(own_key, 6)
    for position, parts in cuts:
        heights = jnp.exp(jax.random.uniform(jax.random.fold_in(own, position), (parts,), jnp.float32, least / len(cuts), high / len(cuts)))
        level = level * jnp.repeat(heights, shape[position] // parts).reshape([-1 if axis == position else 1 for axis in range(len(shape))])
    return level


def gaussian(own_key, dims, spread, most, cuts=(), held_as=jnp.bfloat16):
    loudness = block_levels(own_key, dims, cuts, -0.22, 0.18) if cuts else 1.0
    values = jax.random.normal(own_key, dims, jnp.float32) * spread * loudness
    return jnp.minimum(jnp.maximum(values, -most), most).astype(held_as)


def setup_inputs(seed: int = 0) -> dict:
    streams_of = jax.random.split(jax.random.key(seed), 7)
    prognostic = gaussian(streams_of[0], (3, ELEMENTS, 16, LEV), 1.0, 4.0, ((1, 32),))
    metric = draw_metric(jax.random.fold_in(streams_of[6], 71), 0)
    coriolis = jnp.clip(jax.random.uniform(streams_of[2], (ELEMENTS, 16), jnp.float32, -1.5, 1.5) * block_levels(streams_of[2], (ELEMENTS, 16), ((0, 32),), -0.4, 0.0), -1.5, 1.5)
    node_point = draw_node_point(jax.random.fold_in(streams_of[6], 71), 0)
    send_point = draw_send_point(jax.random.fold_in(streams_of[6], 71), 0)
    recv_point = draw_recv_point(jax.random.fold_in(streams_of[6], 71), 0)
    return dict(prognostic=prognostic, metric=metric, coriolis=coriolis, node_point=node_point, send_point=send_point, recv_point=recv_point)


STEP_SIZE = 0.1

def gll_tables():
    abscissa = np.array([-1.0, -math.sqrt(0.2), math.sqrt(0.2), 1.0])
    legendre = 0.5 * (5.0 * abscissa * abscissa * abscissa - 3.0 * abscissa)
    derivative = np.zeros((4, 4))
    for target in range(4):
        for source in range(4):
            if target != source:
                derivative[target, source] = legendre[target] / (legendre[source] * (abscissa[target] - abscissa[source]))
    derivative[0, 0] = -3.0
    derivative[3, 3] = 3.0
    weights = np.array([1.0, 5.0, 5.0, 1.0]) / 6.0
    return (derivative, weights)

def along_cols(values, derivative):
    return jnp.einsum('aj,erjl->eral', derivative, values, precision=lax.Precision.HIGHEST)

def along_rows(values, derivative):
    return jnp.einsum('aj,ejcl->eacl', derivative, values, precision=lax.Precision.HIGHEST)

def element_tendency(fields, metric, coriolis):
    elements = fields.shape[1]
    levels = fields.shape[3]
    deriv_table, weight_table = gll_tables()
    derivative = jnp.asarray(deriv_table, dtype=jnp.float32)
    weights = jnp.asarray(weight_table, dtype=jnp.float32)
    shaped = fields.reshape(3, elements, 4, 4, levels)
    veloc_one = shaped[0]
    veloc_two = shaped[1]
    geopot = shaped[2]
    inverse = metric.reshape(4, elements, 4, 4, 1)
    inv_aa = inverse[0]
    inv_ab = inverse[1]
    inv_ba = inverse[2]
    inv_bb = inverse[3]
    jacobian_inv = inv_aa * inv_bb - inv_ab * inv_ba
    energy = 0.5 * (veloc_one * veloc_one + veloc_two * veloc_two) + geopot
    ref_one = along_cols(energy, derivative)
    ref_two = along_rows(energy, derivative)
    grad_one = inv_aa * ref_one + inv_ba * ref_two
    grad_two = inv_ab * ref_one + inv_bb * ref_two
    cov_one = (inv_bb * veloc_one - inv_ba * veloc_two) / jacobian_inv
    cov_two = (inv_aa * veloc_two - inv_ab * veloc_one) / jacobian_inv
    vorticity = jacobian_inv * (along_cols(cov_two, derivative) - along_rows(cov_one, derivative))
    absolute = vorticity + coriolis.reshape(elements, 4, 4, 1)
    flux_one = geopot * veloc_one
    flux_two = geopot * veloc_two
    contra_one = (inv_aa * flux_one + inv_ab * flux_two) / jacobian_inv
    contra_two = (inv_ba * flux_one + inv_bb * flux_two) / jacobian_inv
    divergence = jacobian_inv * (along_cols(contra_one, derivative) + along_rows(contra_two, derivative))
    tendency = jnp.stack([absolute * veloc_two - grad_one, -absolute * veloc_one - grad_two, -divergence])
    mass_weight = (weights[:, None] * weights[None, :])[None] / jacobian_inv[..., 0]
    return (tendency.reshape(3, elements, 16, levels), mass_weight.reshape(elements, 16))

def link_groups(lap_blocks):
    side_points = 3 * BY + 1
    top_points = 3 * BX + 1
    group_sizes = [(1, side_points), (-1, side_points), (lap_blocks, top_points), (-lap_blocks, top_points), (lap_blocks + 1, 1), (-lap_blocks - 1, 1), (lap_blocks - 1, 1), (1 - lap_blocks, 1)]
    groups = []
    first_slot = 0
    for offset, slot_count in group_sizes:
        groups.append((offset, first_slot, slot_count))
        first_slot = first_slot + slot_count
    return groups

def block_terms(prognostic, metric, coriolis, node_point, device_index):
    first_elem = (device_index * ELEMS).astype(jnp.int32)
    fields = lax.dynamic_slice_in_dim(prognostic, first_elem, ELEMS, 1).astype(jnp.float32)
    local_metric = lax.dynamic_slice_in_dim(metric, first_elem, ELEMS, 1)
    local_coriolis = lax.dynamic_slice_in_dim(coriolis, first_elem, ELEMS, 0)
    point_ids = lax.dynamic_slice_in_dim(node_point, first_elem, ELEMS, 0).reshape(-1)
    tendency, mass_weight = element_tendency(fields, local_metric, local_coriolis)
    weighted = (tendency * mass_weight[None, :, :, None]).reshape(3, ELEMS * 16, LEV)
    partial_value = jnp.zeros((3, PTS, LEV), jnp.float32).at[:, point_ids, :].add(weighted)
    weight = jnp.zeros((PTS,), jnp.float32).at[point_ids].add(mass_weight.reshape(-1))
    return (fields, point_ids, partial_value, weight)

def reference(prognostic, metric, coriolis, node_point, send_point, recv_point):
    device_list = jnp.arange(BLOCKS, dtype=jnp.int32)

    def outgoing_of(device_index):
        fields, point_ids, partial_value, weight = block_terms(prognostic, metric, coriolis, node_point, device_index)
        link_ids = lax.dynamic_slice_in_dim(send_point, (device_index * LINKS).astype(jnp.int32), LINKS, 0)
        return (partial_value[:, link_ids, :], weight[link_ids])
    sent_values, sent_weight = lax.map(outgoing_of, device_list)
    groups = link_groups(LAP)

    def advance(device_index, collected):
        fields, point_ids, partial_value, weight = block_terms(prognostic, metric, coriolis, node_point, device_index)
        link_ids = lax.dynamic_slice_in_dim(recv_point, (device_index * LINKS).astype(jnp.int32), LINKS, 0)
        arrived_values = []
        arrived_weight = []
        for offset, first_slot, slot_count in groups:
            source = jnp.mod(device_index - offset, BLOCKS).astype(jnp.int32)
            values_from = lax.dynamic_index_in_dim(sent_values, source, 0, keepdims=False)
            weight_from = lax.dynamic_index_in_dim(sent_weight, source, 0, keepdims=False)
            arrived_values.append(values_from[:, first_slot:first_slot + slot_count, :])
            arrived_weight.append(weight_from[first_slot:first_slot + slot_count])
        total = partial_value.at[:, link_ids, :].add(jnp.concatenate(arrived_values, axis=1))
        total_weight = weight.at[link_ids].add(jnp.concatenate(arrived_weight, axis=0))
        averaged = total[:, point_ids, :] / total_weight[point_ids][None, :, None]
        advanced = (fields + STEP_SIZE * averaged.reshape(3, ELEMS, 16, LEV)).astype(jnp.bfloat16)
        first_elem = (device_index * ELEMS).astype(jnp.int32)
        return lax.dynamic_update_slice_in_dim(collected, advanced, first_elem, 1)
    result = jnp.zeros((3, ELEMENTS, 16, LEV), jnp.bfloat16)
    return lax.fori_loop(0, BLOCKS, advance, result)
```

```python
import functools
import math

import jax
import jax.numpy as jnp
import numpy as np
from jax import lax
from jax.experimental import pallas as pl
from jax.experimental.pallas import tpu as pltpu
from jax.sharding import PartitionSpec as P

BX = 32
BY = 2
STEP_SIZE = 0.1
ROWS = 256
LANES = 128
F32 = jnp.float32
BF16 = jnp.bfloat16
MESH = pl.DeviceIdType.MESH


def gll_tables():
    abscissa = np.array([-1.0, -math.sqrt(0.2), math.sqrt(0.2), 1.0])
    legendre = 0.5 * (5.0 * abscissa * abscissa * abscissa - 3.0 * abscissa)
    derivative = np.zeros((4, 4))
    for target in range(4):
        for source in range(4):
            if target != source:
                derivative[target, source] = legendre[target] / (
                    legendre[source] * (abscissa[target] - abscissa[source])
                )
    derivative[0, 0] = -3.0
    derivative[3, 3] = 3.0
    weights = np.array([1.0, 5.0, 5.0, 1.0]) / 6.0
    return (derivative, weights)


def round_bf16(values):
    return np.asarray(values, dtype=jnp.bfloat16).astype(np.float64)


def operator_tables():
    derivative, weights = gll_tables()
    eye4 = np.eye(4)
    node_weight = np.kron(weights, weights)
    along_c = node_weight[:, None] * np.kron(eye4, derivative)
    along_r = node_weight[:, None] * np.kron(derivative, eye4)
    best = None
    for trial in np.linspace(1.0, 2.0, 2001)[:-1]:
        error = max(
            np.max(np.abs(round_bf16(trial * t) / trial - t) / (np.abs(t).max(1, keepdims=True)))
            for t in (along_c, along_r)
        )
        if best is None or error < best[0]:
            best = (error, trial)
    scale = float(best[1])
    eye = np.eye(ROWS // 16)
    stacked = np.concatenate([np.kron(eye, along_c), np.kron(eye, along_r)], axis=0) * scale
    return np.asarray(stacked, dtype=np.float32), scale


def link_groups(lap_blocks):
    side_points = 3 * BY + 1
    top_points = 3 * BX + 1
    group_sizes = [
        (1, side_points),
        (-1, side_points),
        (lap_blocks, top_points),
        (-lap_blocks, top_points),
        (lap_blocks + 1, 1),
        (-lap_blocks - 1, 1),
        (lap_blocks - 1, 1),
        (1 - lap_blocks, 1),
    ]
    groups = []
    first_slot = 0
    first_row = 0
    for offset, slot_count in group_sizes:
        padded = -(-slot_count // 8) * 8
        groups.append((offset, first_slot, slot_count, first_row, padded))
        first_slot += slot_count
        first_row += padded
    return groups, first_row


def iota(shape, dim):
    return lax.broadcasted_iota(jnp.int32, shape, dim)


def dot(a, b):
    return lax.dot_general(a, b, (((1,), (0,)), ((), ())), preferred_element_type=F32)


def dot_nt(a, b):
    return lax.dot_general(a, b, (((1,), (1,)), ((), ())), preferred_element_type=F32)


def kernel(
    sizes, groups, slots, scale,
    prog_hbm, metric_hbm, cor_hbm, node_hbm, send_hbm, recv_hbm, ops_hbm,
    out_hbm,
    prog, metric, cor, node, sendp, recvp, ops,
    wide, weighted, summed, inverse, table_s, table_r,
    outgoing, arrived, out_mass, arrived_mass, result,
    in_sem, out_sem, send_sem, recv_sem, msend_sem, mrecv_sem,
):
    nface, nsub = sizes
    total = nface * nsub
    nodes = prog.shape[1]
    blocks = nodes // ROWS
    me = lax.axis_index("face") * nsub + lax.axis_index("sub")
    peers = []
    for offset, *_ in groups:
        other = lax.rem(me + (offset % total), total)
        peers.append((other // nsub, lax.rem(other, nsub)))

    barrier = pltpu.get_barrier_semaphore()
    for peer in peers:
        pl.semaphore_signal(barrier, inc=1, device_id=peer, device_id_type=MESH)

    loads = []
    for k, (src, dst) in enumerate((
        (metric_hbm, metric), (cor_hbm, cor), (node_hbm, node),
        (send_hbm, sendp), (recv_hbm, recvp), (prog_hbm, prog), (ops_hbm, ops),
    )):
        copy = pltpu.make_async_copy(src, dst, in_sem.at[k])
        copy.start()
        loads.append(copy)
    for copy in loads[:5]:
        copy.wait()

    elements = node.shape[1]
    a, b, e, g = metric[0], metric[1], metric[2], metric[3]
    inv_det = 1.0 / (a * g - b * e)
    lane16 = iota((16, 1), 0)
    col, row = lane16 & 3, lane16 >> 2
    w_node = jnp.where((col == 0) | (col == 3), 1 / 6, 5 / 6) * jnp.where((row == 0) | (row == 3), 1 / 6, 5 / 6)
    mass = w_node * inv_det
    compact = jnp.concatenate(
        [a * inv_det, b * inv_det, e * inv_det, g * inv_det, scale * (mass * cor[...]), mass,
         node[...].astype(F32), jnp.zeros((16, elements), F32)], axis=0).T
    upper = compact.astype(BF16).astype(F32)
    both = jnp.concatenate([upper, compact - upper], axis=1)
    own = (iota((16, 2 * LANES), 1) & 15) == iota((16, 2 * LANES), 0)
    spread = jnp.where(own[None], jnp.broadcast_to(both[:, None, :], (elements, 16, 2 * LANES)), 0.0)
    spread = spread.reshape(nodes, 2 * LANES).astype(BF16)
    pick_l = (iota((2 * LANES, 7 * LANES), 0) & (LANES - 1)) >> 4
    pick = (pick_l == (iota((2 * LANES, 7 * LANES), 1) >> 7)).astype(F32).astype(BF16)
    row_l = (iota((8, 2 * LANES), 1) & (LANES - 1)) >> 4
    point_row = dot_nt((row_l == 6).astype(F32).astype(BF16), spread)[0:1]
    mass_row = dot_nt((row_l == 5).astype(F32).astype(BF16), spread).astype(BF16)
    wide[...] = dot(spread, pick)
    weighted[:, 3 * LANES:] = wide[:, 5 * LANES:6 * LANES].astype(BF16)

    count = sendp.shape[1]
    padded = iota((slots, 1), 0)
    slot_of = jnp.full((slots, 1), -1, jnp.int32)
    for _, first_slot, slot_count, first_row, _ in groups:
        inside = (padded >= first_row) & (padded < first_row + slot_count)
        slot_of = jnp.where(inside, padded - first_row + first_slot, slot_of)
    chosen = slot_of == iota((slots, count), 1)
    vacant = jnp.where(slot_of < 0, -1.0, 0.0)
    send_col = jnp.sum(jnp.where(chosen, sendp[...].astype(F32), 0.0), axis=1, keepdims=True) + vacant
    recv_col = jnp.sum(jnp.where(chosen, recvp[...].astype(F32), 0.0), axis=1, keepdims=True) + vacant
    same = iota((slots, slots), 0) == iota((slots, slots), 1)
    recv_row = jnp.sum(jnp.where(same, recv_col, 0.0), axis=0, keepdims=True)
    table_s[...] = jnp.where(send_col == point_row, 1.0, 0.0).astype(BF16)
    out_mass[...] = dot_nt(mass_row, table_s[...])

    pl.semaphore_wait(barrier, len(peers))
    sends = []
    mass_copies = []
    for k in range(len(groups)):
        copy = pltpu.make_async_remote_copy(
            src_ref=out_mass, dst_ref=arrived_mass.at[k],
            send_sem=msend_sem.at[k], recv_sem=mrecv_sem.at[k],
            device_id=peers[k], device_id_type=MESH)
        copy.start()
        mass_copies.append(copy)
    order = [k for k in range(len(groups)) if k not in (2, 3)] + [2, 3]

    def field_copy(field, k):
        first_row, size = groups[k][3], groups[k][4]
        return pltpu.make_async_remote_copy(
            src_ref=outgoing.at[field, pl.ds(first_row, size)],
            dst_ref=arrived.at[field, pl.ds(first_row, size)],
            send_sem=send_sem.at[field, k], recv_sem=recv_sem.at[field, k],
            device_id=peers[k], device_id_type=MESH)

    copies = {}

    def send_field(field):
        for k in order:
            copies[field, k] = field_copy(field, k)
            copies[field, k].start()

    loads[5].wait()
    loads[6].wait()
    along_c = ops[:ROWS]
    along_r = ops[ROWS:]

    def read(block):
        rows = pl.ds(block * ROWS, ROWS)
        fields = [prog[f, rows].astype(F32) for f in range(3)]
        coefs = [wide[rows, k * LANES:(k + 1) * LANES] for k in range(5)]
        return rows, fields, coefs

    for pair in range(0, blocks, 2):
        one, two = [], []
        for block in (pair, pair + 1):
            _, (u1, u2, phi), (ca, cb, ce, cg, _) = read(block)
            one.append((phi * (ca * u1 + cb * u2)).astype(BF16))
            two.append((phi * (ce * u1 + cg * u2)).astype(BF16))
        div = dot(along_c, jnp.concatenate(one, axis=1)) + dot(along_r, jnp.concatenate(two, axis=1))
        for j, block in enumerate((pair, pair + 1)):
            weighted[pl.ds(block * ROWS, ROWS), 2 * LANES:3 * LANES] = (
                -div[:, j * LANES:(j + 1) * LANES]).astype(BF16)
    outgoing[2] = dot(table_s[...], weighted[:, 2 * LANES:3 * LANES])
    send_field(2)

    for pair in range(0, blocks, 2):
        one, two, energy = [], [], []
        for block in (pair, pair + 1):
            _, (u1, u2, phi), (ca, cb, ce, cg, _) = read(block)
            one.append((ca * u2 - cb * u1).astype(BF16))
            two.append((ce * u2 - cg * u1).astype(BF16))
            energy.append((0.5 * (u1 * u1 + u2 * u2) + phi).astype(BF16))
        energy = jnp.concatenate(energy, axis=1)
        vort = dot(along_c, jnp.concatenate(one, axis=1)) + dot(along_r, jnp.concatenate(two, axis=1))
        ref1 = dot(along_c, energy)
        ref2 = dot(along_r, energy)
        for j, block in enumerate((pair, pair + 1)):
            rows, (u1, u2, _), (ca, cb, ce, cg, cf) = read(block)
            lanes = slice(j * LANES, (j + 1) * LANES)
            eta = vort[:, lanes] + cf
            x1, x2 = ref1[:, lanes], ref2[:, lanes]
            weighted[rows, 0:LANES] = (eta * u2 - (ca * x1 + ce * x2)).astype(BF16)
            weighted[rows, LANES:2 * LANES] = (-(eta * u1) - (cb * x1 + cg * x2)).astype(BF16)
    pair_out = dot(table_s[...], weighted[:, 0:2 * LANES])
    outgoing[0] = pair_out[:, :LANES]
    outgoing[1] = pair_out[:, LANES:]
    send_field(0)
    send_field(1)

    for block in range(blocks):
        rows = pl.ds(block * ROWS, ROWS)
        point = wide[rows, 6 * LANES:7 * LANES][:, 0:1]
        meet = jnp.where(point == point_row, 1.0, 0.0).astype(BF16)
        summed[rows, :] = dot(meet, weighted[...])

    for copy in mass_copies:
        copy.wait_recv()
    lane = iota((1, slots), 1)
    mass_in = jnp.zeros((1, slots), F32)
    for k, (_, _, _, first_row, size) in enumerate(groups):
        inside = (lane >= first_row) & (lane < first_row + size)
        mass_in = jnp.where(inside, arrived_mass[k, 0:1, :], mass_in)
    ones = jnp.ones((slots, LANES), BF16)
    for block in range(blocks):
        rows = pl.ds(block * ROWS, ROWS)
        point = wide[rows, 6 * LANES:7 * LANES][:, 0:1]
        hit = point == recv_row
        table_r[rows, :] = jnp.where(hit, 1.0, 0.0).astype(BF16)
        far = dot(jnp.where(hit, mass_in, 0.0).astype(BF16), ones)
        inv = (STEP_SIZE / scale) / (summed[rows, 3 * LANES:] + far)
        inverse[rows, :] = inv
        for f in range(3):
            lanes = slice(f * LANES, (f + 1) * LANES)
            summed[rows, lanes] = prog[f, rows].astype(F32) + inv * summed[rows, lanes]

    stores = []
    for f in (2, 0, 1):
        for k in order:
            copies[f, k].wait_recv()
        landed = arrived[f].astype(BF16)
        for block in range(blocks):
            rows = pl.ds(block * ROWS, ROWS)
            far = dot(table_r[rows, :], landed)
            value = summed[rows, f * LANES:(f + 1) * LANES] + inverse[rows, :] * far
            result[f, rows] = value.astype(BF16)
        copy = pltpu.make_async_copy(result.at[f], out_hbm.at[f], out_sem.at[f])
        copy.start()
        stores.append(copy)
    for copy in mass_copies:
        copy.wait_send()
    for copy in copies.values():
        copy.wait_send()
    for copy in stores:
        copy.wait()


def local(prognostic, metric, coriolis, node_point, send_point, recv_point):
    elements, per, levels = prognostic.shape[1:]
    nodes = elements * per
    sizes = (lax.axis_size("face"), lax.axis_size("sub"))
    groups, slots = link_groups(4 * sizes[1])
    tables, scale = operator_tables()
    links = send_point.shape[0]
    any_spec = pl.BlockSpec(memory_space=pl.ANY)
    dma = pltpu.SemaphoreType.DMA
    vmem = pltpu.VMEM
    out = pl.pallas_call(
        functools.partial(kernel, sizes, groups, slots, scale),
        out_shape=jax.ShapeDtypeStruct((3, nodes, levels), BF16),
        in_specs=[any_spec] * 7,
        out_specs=any_spec,
        scratch_shapes=[
            vmem((3, nodes, levels), BF16),
            vmem((4, per, elements), F32),
            vmem((per, elements), F32),
            vmem((per, elements), jnp.int32),
            vmem((1, links), jnp.int32),
            vmem((1, links), jnp.int32),
            vmem((2 * ROWS, ROWS), BF16),
            vmem((nodes, 7 * LANES), F32),
            vmem((nodes, 4 * LANES), BF16),
            vmem((nodes, 4 * LANES), F32),
            vmem((nodes, LANES), F32),
            vmem((slots, nodes), BF16),
            vmem((nodes, slots), BF16),
            vmem((3, slots, levels), F32),
            vmem((3, slots, levels), F32),
            vmem((8, slots), F32),
            vmem((len(groups), 8, slots), F32),
            vmem((3, nodes, levels), BF16),
            dma((7,)),
            dma((3,)),
            dma((3, len(groups))),
            dma((3, len(groups))),
            dma((len(groups),)),
            dma((len(groups),)),
        ],
        compiler_params=pltpu.CompilerParams(collective_id=0, has_side_effects=True),
    )(
        prognostic.reshape(3, nodes, levels), metric.swapaxes(1, 2), coriolis.T, node_point.T,
        send_point.reshape(1, links), recv_point.reshape(1, links),
        jnp.asarray(tables, dtype=BF16),
    )
    return out.reshape(3, elements, per, levels)


def solution(mesh):
    placed = (
        P(None, ("face", "sub"), None, None),
        P(None, ("face", "sub"), None),
        P(("face", "sub"), None),
        P(("face", "sub"), None),
        P(("face", "sub")),
        P(("face", "sub")),
    )
    return jax.shard_map(
        local,
        mesh=mesh,
        in_specs=placed,
        out_specs=P(None, ("face", "sub"), None, None),
        check_vma=False,
    )
```

```python
import functools
import math

import jax
import jax.numpy as jnp
import numpy as np
from jax import lax
from jax.experimental import pallas as pl
from jax.experimental.pallas import tpu as pltpu
from jax.sharding import PartitionSpec as P

BX = 32
BY = 2
STEP_SIZE = 0.1
ROWS = 256
LANES = 128
F32 = jnp.float32
BF16 = jnp.bfloat16
MESH = pl.DeviceIdType.MESH


def gll_tables():
    abscissa = np.array([-1.0, -math.sqrt(0.2), math.sqrt(0.2), 1.0])
    legendre = 0.5 * (5.0 * abscissa * abscissa * abscissa - 3.0 * abscissa)
    derivative = np.zeros((4, 4))
    for target in range(4):
        for source in range(4):
            if target != source:
                derivative[target, source] = legendre[target] / (
                    legendre[source] * (abscissa[target] - abscissa[source])
                )
    derivative[0, 0] = -3.0
    derivative[3, 3] = 3.0
    weights = np.array([1.0, 5.0, 5.0, 1.0]) / 6.0
    return (derivative, weights)


def round_bf16(values):
    return np.asarray(values, dtype=jnp.bfloat16).astype(np.float64)


def operator_tables():
    derivative, weights = gll_tables()
    eye4 = np.eye(4)
    node_weight = np.kron(weights, weights)
    along_c = node_weight[:, None] * np.kron(eye4, derivative)
    along_r = node_weight[:, None] * np.kron(derivative, eye4)
    best = None
    for trial in np.linspace(1.0, 2.0, 2001)[:-1]:
        error = max(
            np.max(np.abs(round_bf16(trial * t) / trial - t) / (np.abs(t).max(1, keepdims=True)))
            for t in (along_c, along_r)
        )
        if best is None or error < best[0]:
            best = (error, trial)
    scale = float(best[1])
    eye = np.eye(ROWS // 16)
    stacked = np.concatenate([np.kron(eye, along_c), np.kron(eye, along_r)], axis=0) * scale
    return np.asarray(stacked, dtype=np.float32), scale


def link_groups(lap_blocks):
    side_points = 3 * BY + 1
    top_points = 3 * BX + 1
    group_sizes = [
        (1, side_points),
        (-1, side_points),
        (lap_blocks, top_points),
        (-lap_blocks, top_points),
        (lap_blocks + 1, 1),
        (-lap_blocks - 1, 1),
        (lap_blocks - 1, 1),
        (1 - lap_blocks, 1),
    ]
    groups = []
    first_slot = 0
    first_row = 0
    for offset, slot_count in group_sizes:
        padded = -(-slot_count // 8) * 8
        groups.append((offset, first_slot, slot_count, first_row, padded))
        first_slot += slot_count
        first_row += padded
    return groups, first_row


def iota(shape, dim):
    return lax.broadcasted_iota(jnp.int32, shape, dim)


def dot(a, b):
    return lax.dot_general(a, b, (((1,), (0,)), ((), ())), preferred_element_type=F32)


def dot_nt(a, b):
    return lax.dot_general(a, b, (((1,), (1,)), ((), ())), preferred_element_type=F32)


def wait_bytes(ref, sem):
    pltpu.make_async_copy(ref, ref, sem).wait()


def kernel(
    sizes, groups, slots, scale,
    prog_hbm, metric_hbm, cor_hbm, node_hbm, send_hbm, recv_hbm, ops_hbm,
    out_hbm,
    prog, metric, cor, node, sendp, recvp, ops,
    wide, weighted, summed, inverse, table_s, table_r,
    outgoing, arrived, out_mass, arrived_mass,
    in_sem, send_sem, recv_sem, msend_sem, mrecv_sem,
):
    nface, nsub = sizes
    total = nface * nsub
    nodes = prog.shape[1]
    blocks = nodes // ROWS
    me = lax.axis_index("face") * nsub + lax.axis_index("sub")
    peers = []
    for offset, *_ in groups:
        other = lax.rem(me + (offset % total), total)
        peers.append((other // nsub, lax.rem(other, nsub)))

    arrived[...] = jnp.zeros_like(arrived)
    barrier = pltpu.get_barrier_semaphore()
    for peer in peers:
        pl.semaphore_signal(barrier, inc=1, device_id=peer, device_id_type=MESH)

    loads = []
    for k, (src, dst) in enumerate((
        (metric_hbm, metric), (cor_hbm, cor), (node_hbm, node),
        (send_hbm, sendp), (recv_hbm, recvp), (prog_hbm, prog), (ops_hbm, ops),
    )):
        copy = pltpu.make_async_copy(src, dst, in_sem.at[k])
        copy.start()
        loads.append(copy)
    for copy in loads[:5]:
        copy.wait()

    elements = node.shape[1]
    a, b, e, g = metric[0], metric[1], metric[2], metric[3]
    inv_det = 1.0 / (a * g - b * e)
    lane16 = iota((16, 1), 0)
    col, row = lane16 & 3, lane16 >> 2
    w_node = jnp.where((col == 0) | (col == 3), 1 / 6, 5 / 6) * jnp.where((row == 0) | (row == 3), 1 / 6, 5 / 6)
    mass = w_node * inv_det
    compact = jnp.concatenate(
        [a * inv_det, b * inv_det, e * inv_det, g * inv_det, scale * (mass * cor[...]), mass,
         node[...].astype(F32), jnp.zeros((16, elements), F32)], axis=0).T
    upper = compact.astype(BF16).astype(F32)
    both = jnp.concatenate([upper, compact - upper], axis=1)
    own = (iota((16, 2 * LANES), 1) & 15) == iota((16, 2 * LANES), 0)
    spread = jnp.where(own[None], jnp.broadcast_to(both[:, None, :], (elements, 16, 2 * LANES)), 0.0)
    spread = spread.reshape(nodes, 2 * LANES).astype(BF16)
    pick_l = (iota((2 * LANES, 7 * LANES), 0) & (LANES - 1)) >> 4
    pick = (pick_l == (iota((2 * LANES, 7 * LANES), 1) >> 7)).astype(F32).astype(BF16)
    row_l = (iota((8, 2 * LANES), 1) & (LANES - 1)) >> 4
    point_row = dot_nt((row_l == 6).astype(F32).astype(BF16), spread)[0:1]
    mass_row = dot_nt((row_l == 5).astype(F32).astype(BF16), spread).astype(BF16)
    wide[...] = dot(spread, pick)
    weighted[:, 3 * LANES:] = wide[:, 5 * LANES:6 * LANES].astype(BF16)

    count = sendp.shape[1]
    padded = iota((slots, 1), 0)
    slot_of = jnp.full((slots, 1), -1, jnp.int32)
    for _, first_slot, slot_count, first_row, _ in groups:
        inside = (padded >= first_row) & (padded < first_row + slot_count)
        slot_of = jnp.where(inside, padded - first_row + first_slot, slot_of)
    chosen = slot_of == iota((slots, count), 1)
    vacant = jnp.where(slot_of < 0, -1.0, 0.0)
    send_col = jnp.sum(jnp.where(chosen, sendp[...].astype(F32), 0.0), axis=1, keepdims=True) + vacant
    recv_col = jnp.sum(jnp.where(chosen, recvp[...].astype(F32), 0.0), axis=1, keepdims=True) + vacant
    same = iota((slots, slots), 0) == iota((slots, slots), 1)
    recv_row = jnp.sum(jnp.where(same, recv_col, 0.0), axis=0, keepdims=True)
    table_s[...] = jnp.where(send_col == point_row, 1.0, 0.0).astype(BF16)
    out_mass[...] = dot_nt(mass_row, table_s[...])[0:1]

    pl.semaphore_wait(barrier, len(peers))
    for k in range(len(groups)):
        copy = pltpu.make_async_remote_copy(
            src_ref=out_mass, dst_ref=arrived_mass.at[k],
            send_sem=msend_sem.at[0], recv_sem=mrecv_sem.at[0],
            device_id=peers[k], device_id_type=MESH)
        copy.start()
    order = [k for k in range(len(groups)) if k not in (2, 3)] + [2, 3]

    def field_copy(field, k):
        used, first_row = groups[k][2], groups[k][3]
        return pltpu.make_async_remote_copy(
            src_ref=outgoing.at[field, pl.ds(first_row, used)],
            dst_ref=arrived.at[field, pl.ds(first_row, used)],
            send_sem=send_sem.at[field], recv_sem=recv_sem.at[field],
            device_id=peers[k], device_id_type=MESH)

    def send_field(field):
        for k in order:
            field_copy(field, k).start()

    loads[5].wait()
    loads[6].wait()
    along_c = ops[:ROWS]
    along_r = ops[ROWS:]

    def read(block):
        rows = pl.ds(block * ROWS, ROWS)
        fields = [prog[f, rows].astype(F32) for f in range(3)]
        coefs = [wide[rows, k * LANES:(k + 1) * LANES] for k in range(5)]
        return rows, fields, coefs

    for pair in range(0, blocks, 2):
        one, two = [], []
        for block in (pair, pair + 1):
            _, (u1, u2, phi), (ca, cb, ce, cg, _) = read(block)
            one.append((phi * (ca * u1 + cb * u2)).astype(BF16))
            two.append((phi * (ce * u1 + cg * u2)).astype(BF16))
        div = dot(along_c, jnp.concatenate(one, axis=1)) + dot(along_r, jnp.concatenate(two, axis=1))
        for j, block in enumerate((pair, pair + 1)):
            weighted[pl.ds(block * ROWS, ROWS), 2 * LANES:3 * LANES] = (
                -div[:, j * LANES:(j + 1) * LANES]).astype(BF16)
    outgoing[2] = dot(table_s[...], weighted[:, 2 * LANES:3 * LANES])
    send_field(2)

    for pair in range(0, blocks, 2):
        one, two, energy = [], [], []
        for block in (pair, pair + 1):
            _, (u1, u2, phi), (ca, cb, ce, cg, _) = read(block)
            one.append((ca * u2 - cb * u1).astype(BF16))
            two.append((ce * u2 - cg * u1).astype(BF16))
            energy.append((0.5 * (u1 * u1 + u2 * u2) + phi).astype(BF16))
        energy = jnp.concatenate(energy, axis=1)
        vort = dot(along_c, jnp.concatenate(one, axis=1)) + dot(along_r, jnp.concatenate(two, axis=1))
        ref1 = dot(along_c, energy)
        ref2 = dot(along_r, energy)
        for j, block in enumerate((pair, pair + 1)):
            rows, (u1, u2, _), (ca, cb, ce, cg, cf) = read(block)
            lanes = slice(j * LANES, (j + 1) * LANES)
            eta = vort[:, lanes] + cf
            x1, x2 = ref1[:, lanes], ref2[:, lanes]
            weighted[rows, 0:LANES] = (eta * u2 - (ca * x1 + ce * x2)).astype(BF16)
            weighted[rows, LANES:2 * LANES] = (-(eta * u1) - (cb * x1 + cg * x2)).astype(BF16)
    pair_out = dot(table_s[...], weighted[:, 0:2 * LANES])
    outgoing[0] = pair_out[:, :LANES]
    outgoing[1] = pair_out[:, LANES:]
    send_field(0)
    send_field(1)

    for block in range(blocks):
        rows = pl.ds(block * ROWS, ROWS)
        point = wide[rows, 6 * LANES:7 * LANES][:, 0:1]
        meet = jnp.where(point == point_row, 1.0, 0.0).astype(BF16)
        summed[rows, :] = dot(meet, weighted[...])

    wait_bytes(arrived_mass, mrecv_sem.at[0])
    lane = iota((1, slots), 1)
    mass_in = jnp.zeros((1, slots), F32)
    for k, (_, _, _, first_row, size) in enumerate(groups):
        inside = (lane >= first_row) & (lane < first_row + size)
        mass_in = jnp.where(inside, arrived_mass[k, 0:1, :], mass_in)
    ones = jnp.ones((slots, LANES), BF16)
    for block in range(blocks):
        rows = pl.ds(block * ROWS, ROWS)
        point = wide[rows, 6 * LANES:7 * LANES][:, 0:1]
        hit = point == recv_row
        table_r[rows, :] = jnp.where(hit, 1.0, 0.0).astype(BF16)
        far = dot(jnp.where(hit, mass_in, 0.0).astype(BF16), ones)
        inv = (STEP_SIZE / scale) / (summed[rows, 3 * LANES:] + far)
        inverse[rows, :] = inv
        for f in range(3):
            lanes = slice(f * LANES, (f + 1) * LANES)
            summed[rows, lanes] = prog[f, rows].astype(F32) + inv * summed[rows, lanes]

    for f in (2, 0, 1):
        wait_bytes(arrived.at[f, pl.ds(0, count)], recv_sem.at[f])
        landed = arrived[f].astype(BF16)
        for block in range(blocks):
            rows = pl.ds(block * ROWS, ROWS)
            far = dot(table_r[rows, :], landed)
            value = summed[rows, f * LANES:(f + 1) * LANES] + inverse[rows, :] * far
            out_hbm[f, rows] = value
    wait_bytes(arrived_mass, msend_sem.at[0])
    for f in range(3):
        wait_bytes(outgoing.at[f, pl.ds(0, count)], send_sem.at[f])


def local(prognostic, metric, coriolis, node_point, send_point, recv_point):
    elements, per, levels = prognostic.shape[1:]
    nodes = elements * per
    sizes = (lax.axis_size("face"), lax.axis_size("sub"))
    groups, slots = link_groups(4 * sizes[1])
    tables, scale = operator_tables()
    links = send_point.shape[0]
    any_spec = pl.BlockSpec(memory_space=pltpu.HBM)
    dma = pltpu.SemaphoreType.DMA
    vmem = pltpu.VMEM
    out = pl.pallas_call(
        functools.partial(kernel, sizes, groups, slots, scale),
        out_shape=pltpu.VMEM((3, nodes, levels), F32),
        in_specs=[any_spec] * 7,
        out_specs=pl.BlockSpec(memory_space=pltpu.VMEM),
        scratch_shapes=[
            vmem((3, nodes, levels), BF16),
            vmem((4, per, elements), F32),
            vmem((per, elements), F32),
            vmem((per, elements), jnp.int32),
            vmem((1, links), jnp.int32),
            vmem((1, links), jnp.int32),
            vmem((2 * ROWS, ROWS), BF16),
            vmem((nodes, 7 * LANES), F32),
            vmem((nodes, 4 * LANES), BF16),
            vmem((nodes, 4 * LANES), F32),
            vmem((nodes, LANES), F32),
            vmem((slots, nodes), BF16),
            vmem((nodes, slots), BF16),
            vmem((3, slots, levels), F32),
            vmem((3, slots, levels), F32),
            vmem((1, slots), F32),
            vmem((len(groups), 1, slots), F32),
            dma((7,)),
            dma((3,)),
            dma((3,)),
            dma((1,)),
            dma((1,)),
        ],
        compiler_params=pltpu.CompilerParams(
            collective_id=0, has_side_effects=True),
    )(
        prognostic.reshape(3, nodes, levels), metric.swapaxes(1, 2), coriolis.T, node_point.T,
        send_point.reshape(1, links), recv_point.reshape(1, links),
        jnp.asarray(tables, dtype=BF16),
    )
    return out.astype(BF16).reshape(3, elements, per, levels)


def solution(mesh):
    placed = (
        P(None, ("face", "sub"), None, None),
        P(None, ("face", "sub"), None),
        P(("face", "sub"), None),
        P(("face", "sub"), None),
        P(("face", "sub")),
        P(("face", "sub")),
    )
    return jax.shard_map(
        local,
        mesh=mesh,
        in_specs=placed,
        out_specs=P(None, ("face", "sub"), None, None),
        check_vma=False,
    )
```
